32 devices in a mesh: dp: 4 (over x, core), pipe: 4 (over z), tensor: 2 (over y).
Axes of the slice: x: 2, y: 2, z: 4, core: 2. Of those that a mesh axis runs over, the one named last changes fastest.
Arguments:
- support_tokens: int32 [32, 32], P(('dp', 'pipe')), may hold values from 0 to 64127
- support_lengths: int32 [32], P(('dp', 'pipe')), may hold values from 1 to 32
- support_labels: int32 [32, 1], P(('dp', 'pipe')), may hold values from 0 to 31
- query_tokens: int32 [16, 32], P(('dp', 'pipe')), may hold values from 0 to 64127
- query_lengths: int32 [16], P(('dp', 'pipe')), may hold values from 1 to 32
- query_episodes: int32 [16], P(('dp', 'pipe')), may hold values from 0 to 1
- embedding: bfloat16 [64128, 4096], P(('dp', 'pipe'), 'tensor'), may hold values from -18 to 18
- attn_gain: float32 [4, 4096], P('pipe'), may hold values from 0.5 to 1.5
- query_weight: bfloat16 [4, 4096, 4096], P('pipe', None, 'tensor'), may hold values from -1 to 1
- key_weight: bfloat16 [4, 4096, 1024], P('pipe', None, 'tensor'), may hold values from -16 to 16
- value_weight: bfloat16 [4, 4096, 1024], P('pipe', None, 'tensor'), may hold values from -0.09375 to 0.09375
- out_weight: bfloat16 [4, 4096, 4096], P('pipe', 'tensor'), may hold values from -0.09375 to 0.09375
- final_gain: float32 [4096], replicated, may hold values from 0.5 to 1.5
Outputs:
- prototypes: float32 [32, 4096], P(None, 'tensor')
- logits: float32 [16, 16], P(('dp', 'pipe'))
The draws below stay inside these ranges and needn't reach their ends.
Inputs may be any that keep to these rules, and one draw needn't show every extreme that they name: `support_labels`: every class is the label of at least one support sequence.
All inputs are finite; a program needn't handle non-finite values.
Results may differ from the reference program's by a relative error of at most 0.024.
Values may be sent and summed in bfloat16 or wider, within the bound.
No kernel may reach another device: no remote copies, remote signals or barrier semaphores. Data moves between devices by JAX's collectives and lax.ppermute only.
A program may use at most 128 MiB of HBM per device.

```python
import math
import jax
import jax.numpy as jnp
import numpy as np
from jax import lax

D = 4096
HEADS = 32
KV_HEADS = 8
HEAD_DIM = 128
VOCAB = 64128
WAYS = 16
EPISODES = 2
LEN = 32
LAYERS = 4
SUPPORTS = 32
QUERIES = 16
CLASSES = 32
N_TENSOR = 2


def shared_projection(key):
    base = jax.random.normal(jax.random.fold_in(key, 7), (LAYERS, D, HEADS * HEAD_DIM), jnp.float32)
    return jnp.clip(base, -6.0, 6.0) / math.sqrt(D)


def draw_query_weight(key, part):
    return shared_projection(key).astype(jnp.bfloat16)


def draw_key_weight(key, part):
    noise = jax.random.normal(jax.random.fold_in(key, 13), (LAYERS, D, KV_HEADS * HEAD_DIM), jnp.float32)
    noise = jnp.clip(noise, -6.0, 6.0) / math.sqrt(D)
    return noise.astype(jnp.bfloat16)


def draw_embedding(key, part):
    row_scale = jnp.exp(jax.random.uniform(jax.random.fold_in(key, 21), (VOCAB, 1), jnp.float32, math.log(0.3), math.log(3.0)))
    values = jnp.clip(jax.random.normal(jax.random.fold_in(key, 27), (VOCAB, D), jnp.float32), -6.0, 6.0)
    return (values * row_scale).astype(jnp.bfloat16)


def place_ends(entries, rng, low, high):
    extent = entries.shape
    index_at = [jax.random.randint(jax.random.fold_in(rng, axis), (), 0, extent[axis]) for axis in range(len(extent))]
    entries = entries.at[tuple(index_at)].set(low)
    longest = extent.index(max(extent))
    index_at[longest] = (index_at[longest] + 1) % extent[longest]
    return entries.at[tuple(index_at)].set(high)


def steps_of(rng, dims, pieces, least, top_value):
    gain = 1.0
    for axis_at, blocks in pieces:
        steps = jax.random.uniform(jax.random.fold_in(jax.random.fold_in(rng, 6), axis_at), (blocks,), jnp.float32, least / len(pieces), top_value / len(pieces))
        gain = gain * jnp.repeat(jnp.exp(steps), dims[axis_at] // blocks).reshape((-1,) + (1,) * (len(dims) - 1 - axis_at))
    return gain


def cumulative_ranks(number_of, lean):
    portions = [(1 << 20) // math.isqrt(rank ** lean) + 1 for rank in range(1, number_of + 1)]
    spread = 1 + sum(portions) // (1 << 30)
    return np.cumsum(np.array([max(1, weight // spread) for weight in portions]))


def ranked_ids(rng, dims, number_of, slope):
    table = cumulative_ranks(number_of, slope)
    pick = jax.random.randint(jax.random.fold_in(rng, 1), dims, 0, int(table[number_of - 1]))
    standing = jnp.searchsorted(jnp.asarray(table, jnp.int32), pick, side="right")
    return jax.random.permutation(jax.random.fold_in(rng, 2), number_of)[standing].astype(jnp.int32)


def picks_of(rng, rows, amount, top, lift):
    ranking = jax.random.permutation(jax.random.fold_in(rng, 1), amount)
    favour = ranking
    for power in range(3):
        favour = favour * favour // amount
    favour = favour * lift // amount
    lots = jax.random.randint(jax.random.fold_in(rng, 2), (rows, amount), 0, 4096) + favour
    holders = jax.random.permutation(jax.random.fold_in(rng, 3), rows)[jnp.arange(amount) % rows]
    lots = jnp.where(jnp.arange(rows)[:, None] == holders[None, :], 1 << 14, lots)
    score = lots * amount + jnp.arange(amount)
    return lax.top_k(score.astype(jnp.int32), top)[1].astype(jnp.int32)


def gaussian(own_key, extent, scale, most, cuts=(), held_as=jnp.bfloat16):
    values = scale * jax.random.normal(own_key, extent, jnp.float32)
    if cuts:
        values = values * steps_of(own_key, extent, cuts, -0.22, 0.18)
    return jnp.clip(values, -most, most).astype(held_as)


def setup_inputs(seed: int = 0) -> dict:
    key_of = jax.random.split(jax.random.key(seed), 14)
    support_tokens = place_ends(ranked_ids(key_of[0], (SUPPORTS, LEN), VOCAB, 2), jax.random.fold_in(key_of[0], 3), 0, VOCAB - 1).astype(jnp.int32)
    support_lengths = place_ends(jax.random.randint(key_of[1], (SUPPORTS,), 1, LEN + 1), jax.random.fold_in(key_of[1], 1), 1, LEN).astype(jnp.int32)
    support_labels = picks_of(key_of[2], SUPPORTS, CLASSES, 1, 0)
    query_tokens = place_ends(ranked_ids(key_of[3], (QUERIES, LEN), VOCAB, 2), jax.random.fold_in(key_of[3], 3), 0, VOCAB - 1).astype(jnp.int32)
    query_lengths = place_ends(jax.random.randint(key_of[4], (QUERIES,), 1, LEN + 1), jax.random.fold_in(key_of[4], 1), 1, LEN).astype(jnp.int32)
    query_episodes = place_ends(jax.random.randint(key_of[5], (QUERIES,), 0, EPISODES), jax.random.fold_in(key_of[5], 1), 0, EPISODES - 1).astype(jnp.int32)
    embedding = draw_embedding(jax.random.fold_in(key_of[13], 71), 0)
    attn_gain = jnp.clip(1.0 + 0.1 * jax.random.normal(key_of[7], (LAYERS, D), jnp.float32), 0.5, 1.5)
    query_weight = draw_query_weight(jax.random.fold_in(key_of[13], 71), 0)
    key_weight = draw_key_weight(jax.random.fold_in(key_of[13], 71), 0)
    value_weight = gaussian(key_of[10], (LAYERS, D, KV_HEADS * HEAD_DIM), D ** -0.5, 0.09375, ((0, 4), (2, 2)))
    out_weight = gaussian(key_of[11], (LAYERS, HEADS * HEAD_DIM, D), (HEADS * HEAD_DIM) ** -0.5, 0.09375, ((0, 4), (1, 2)))
    final_gain = jnp.clip(1.0 + 0.1 * jax.random.normal(key_of[12], (D,), jnp.float32), 0.5, 1.5)
    return {"support_tokens": support_tokens, "support_lengths": support_lengths, "support_labels": support_labels, "query_tokens": query_tokens, "query_lengths": query_lengths, "query_episodes": query_episodes, "embedding": embedding, "attn_gain": attn_gain, "query_weight": query_weight, "key_weight": key_weight, "value_weight": value_weight, "out_weight": out_weight, "final_gain": final_gain}


epsilon = 1e-05
rotary_base = 500000.0

def normed_values(hidden, gain_vector):
    values = hidden.astype(jnp.float32)
    mean_square = lax.optimization_barrier(jnp.mean(values * values, axis=-1, keepdims=True))
    return values * lax.rsqrt(mean_square + epsilon) * gain_vector.astype(jnp.float32)

def rotate(heads_in, seq_len):
    half_dim = HEAD_DIM // 2
    freqs = jnp.exp(-math.log(rotary_base) * jnp.arange(half_dim, dtype=jnp.float32) * (2.0 / HEAD_DIM))
    angles = jnp.arange(seq_len, dtype=jnp.float32)[:, None] * freqs[None, :]
    cosine = jnp.cos(angles)[None, :, None, :]
    sine = jnp.sin(angles)[None, :, None, :]
    first_half = heads_in[..., :half_dim]
    second_half = heads_in[..., half_dim:]
    return jnp.concatenate([first_half * cosine - second_half * sine, second_half * cosine + first_half * sine], axis=-1)

def attention_block(hidden, gain_vector, query_proj, key_proj, value_proj, out_proj, seq_lengths):
    seq_count, seq_len, width = hidden.shape
    normed = normed_values(hidden, gain_vector).astype(jnp.bfloat16).reshape(seq_count * seq_len, width)
    query_heads = jnp.dot(normed, query_proj, preferred_element_type=jnp.float32).reshape(seq_count, seq_len, HEADS, HEAD_DIM)
    key_heads = jnp.dot(normed, key_proj, preferred_element_type=jnp.float32).reshape(seq_count, seq_len, KV_HEADS, HEAD_DIM)
    value_heads = jnp.dot(normed, value_proj, preferred_element_type=jnp.float32).reshape(seq_count, seq_len, KV_HEADS, HEAD_DIM)
    query_heads = rotate(query_heads, seq_len).astype(jnp.bfloat16)
    key_heads = rotate(key_heads, seq_len).astype(jnp.bfloat16)
    value_heads = value_heads.astype(jnp.bfloat16)
    group_size = HEADS // KV_HEADS
    grouped = query_heads.astype(jnp.float32).reshape(seq_count, seq_len, KV_HEADS, group_size, HEAD_DIM)
    scores = jnp.einsum('sikgd,sjkd->skgij', grouped, key_heads.astype(jnp.float32)) / math.sqrt(HEAD_DIM)
    positions = jnp.arange(seq_len)
    causal = positions[None, :] <= positions[:, None]
    visible = causal[None, :, :] & (positions[None, None, :] < seq_lengths[:, None, None])
    scores = jnp.where(visible[:, None, None, :, :], scores, -1e+30)
    weights = jax.nn.softmax(scores, axis=-1).astype(jnp.bfloat16)
    mixed = jnp.einsum('skgij,sjkd->sikgd', weights.astype(jnp.float32), value_heads.astype(jnp.float32))
    mixed = mixed.astype(jnp.bfloat16).reshape(seq_count * seq_len, HEADS * HEAD_DIM)
    shard_width = HEADS * HEAD_DIM // N_TENSOR
    running = jnp.zeros((seq_count * seq_len, width), jnp.float32)
    for shard_index in range(N_TENSOR):
        low = shard_index * shard_width
        term = jnp.dot(mixed[:, low:low + shard_width], out_proj[low:low + shard_width], preferred_element_type=jnp.float32)
        running = running + lax.optimization_barrier(term.astype(jnp.bfloat16)).astype(jnp.float32)
    updated = hidden.astype(jnp.float32).reshape(seq_count * seq_len, width) + running
    return updated.astype(jnp.bfloat16).reshape(seq_count, seq_len, width)

def reference(support_tokens, support_lengths, support_labels, query_tokens, query_lengths, query_episodes, embedding, attn_gain, query_weight, key_weight, value_weight, out_weight, final_gain):
    token_ids = jnp.concatenate([support_tokens, query_tokens], axis=0)
    seq_lengths = jnp.concatenate([support_lengths, query_lengths], axis=0)
    hidden = jnp.take(embedding, token_ids, axis=0)
    for layer_index in range(LAYERS):
        hidden = attention_block(hidden, attn_gain[layer_index], query_weight[layer_index], key_weight[layer_index], value_weight[layer_index], out_weight[layer_index], seq_lengths)
    final = normed_values(hidden, final_gain)
    live = (jnp.arange(LEN)[None, :] < seq_lengths[:, None]).astype(jnp.float32)
    pooled = lax.optimization_barrier(jnp.sum(final * live[:, :, None], axis=1)) / seq_lengths[:, None].astype(jnp.float32)
    support_pooled = pooled[:SUPPORTS]
    query_pooled = pooled[SUPPORTS:]
    onehot = (support_labels[:, 0][:, None] == jnp.arange(CLASSES)[None, :]).astype(jnp.float32)
    class_total = jnp.dot(onehot.T, support_pooled, precision=lax.Precision.HIGHEST)
    class_count = lax.optimization_barrier(jnp.sum(onehot, axis=0))
    prototypes = class_total / class_count[:, None]
    chosen = prototypes.reshape(EPISODES, WAYS, D)[query_episodes]
    distance = lax.optimization_barrier(jnp.sum((query_pooled[:, None, :] - chosen) ** 2, axis=-1))
    logits = -distance / math.sqrt(D)
    return (prototypes, logits)
```

```python
import functools
import math

import jax
import jax.numpy as jnp
from jax import lax
from jax.experimental import pallas as pl
from jax.experimental.pallas import tpu as pltpu
from jax.sharding import PartitionSpec as P

D = 4096
HEAD_DIM = 128
WAYS = 16
EPISODES = 2
GRANT = 6 * 1024 * 1024
SLOTS = 16
GROUPS = ((0, 1, 2),)

epsilon = 1e-05
rotary_base = 500000.0


def rotary_tables(seq_len):
    half_dim = HEAD_DIM // 2
    freqs = jnp.exp(
        -math.log(rotary_base) * jnp.arange(half_dim, dtype=jnp.float32) * (2.0 / HEAD_DIM)
    )
    angles = jnp.arange(seq_len, dtype=jnp.float32)[:, None] * freqs[None, :]
    cosine, sine = jnp.cos(angles), jnp.sin(angles)
    return (
        jnp.concatenate([cosine, cosine], axis=1),
        jnp.concatenate([-sine, sine], axis=1),
    )


def block_kernel(
    place_ref,
    lengths_ref,
    *refs,
    parts,
    seqs,
    seq_len,
    chunk,
):
    rows_refs = refs[:parts]
    gain_ref, cos_ref, sin_ref, wq_ref, wk_ref, wv_ref, wo_ref = refs[parts : parts + 7]
    out_refs = refs[parts + 7 : 2 * parts + 7]
    qkv_ref, mixed_ref = refs[2 * parts + 7 :]
    width = rows_refs[0].shape[1]
    rows = seqs * seq_len
    here = place_ref[0]
    starts = [pl.multiple_of(lax.rem(here + parts - k, parts) * width, width) for k in range(parts)]
    total = jnp.zeros((rows, 1), jnp.float32)
    for ref in rows_refs:
        values = ref[...].astype(jnp.float32)
        total = total + jnp.sum(values * values, axis=1, keepdims=True)
    scale = lax.rsqrt(total / (parts * width) + epsilon)
    normed = []
    for ref, start in zip(rows_refs, starts):
        gain = gain_ref[:, pl.ds(start, width)]
        normed.append((ref[...].astype(jnp.float32) * scale * gain).astype(jnp.bfloat16))
    query_cols = wq_ref.shape[1]
    key_cols = wk_ref.shape[1]
    cosine = jnp.concatenate([cos_ref[...]] * seqs, axis=0)
    sine = jnp.concatenate([sin_ref[...]] * seqs, axis=0)

    def project(weight_ref, base, turned):
        cols = weight_ref.shape[1]
        step = min(chunk, cols)
        for at in range(0, cols, step):
            acc = None
            for part, start in zip(normed, starts):
                term = jnp.dot(
                    part,
                    weight_ref[pl.ds(start, width), at : at + step],
                    preferred_element_type=jnp.float32,
                )
                acc = term if acc is None else acc + term
            for low in range(0, step, HEAD_DIM):
                head = acc[:, low : low + HEAD_DIM]
                if turned:
                    head = head * cosine + pltpu.roll(head, HEAD_DIM // 2, 1) * sine
                qkv_ref[:, base + at + low : base + at + low + HEAD_DIM] = head.astype(jnp.bfloat16)

    project(wk_ref, query_cols, True)
    project(wv_ref, query_cols + key_cols, False)
    project(wq_ref, 0, True)
    heads = query_cols // HEAD_DIM
    groups = key_cols // HEAD_DIM
    each = heads // groups
    spot = lax.broadcasted_iota(jnp.int32, (each * seq_len, seq_len), 0) % seq_len
    seen = lax.broadcasted_iota(jnp.int32, (each * seq_len, seq_len), 1)
    for s in range(seqs):
        at = slice(s * seq_len, (s + 1) * seq_len)
        visible = (seen <= spot) & (seen < lengths_ref[s])
        for g in range(groups):
            query = jnp.concatenate(
                [
                    qkv_ref[at, (g * each + i) * HEAD_DIM : (g * each + i + 1) * HEAD_DIM]
                    for i in range(each)
                ],
                axis=0,
            )
            key = qkv_ref[at, query_cols + g * HEAD_DIM : query_cols + (g + 1) * HEAD_DIM]
            base = query_cols + key_cols
            value = qkv_ref[at, base + g * HEAD_DIM : base + (g + 1) * HEAD_DIM]
            scores = lax.dot_general(
                query, key, (((1,), (1,)), ((), ())), preferred_element_type=jnp.float32
            ) * (1.0 / math.sqrt(HEAD_DIM))
            scores = jnp.where(visible, scores, -1e30)
            top = jnp.max(scores, axis=1, keepdims=True)
            powers = jnp.exp(scores - top)
            weights = (powers / jnp.sum(powers, axis=1, keepdims=True)).astype(jnp.bfloat16)
            mixed = jnp.dot(weights, value, preferred_element_type=jnp.float32).astype(jnp.bfloat16)
            for i in range(each):
                low = (g * each + i) * HEAD_DIM
                mixed_ref[at, low : low + HEAD_DIM] = mixed[i * seq_len : (i + 1) * seq_len]
    mixed = mixed_ref[...]
    for k in list(range(1, parts)) + [0]:
        to = pl.multiple_of(lax.rem(here + k, parts) * width, width)
        for low in range(0, width, chunk):
            out_refs[k][:, low : low + chunk] = jnp.dot(
                mixed, wo_ref[:, pl.ds(to + low, chunk)], preferred_element_type=jnp.float32
            ).astype(jnp.bfloat16)


def block(place, lengths, pieces, gain, tables, weights, seq_len):
    parts = len(pieces)
    rows, width = pieces[0].shape
    seqs = rows // seq_len
    wq, wk, wv, wo = weights
    cols = wq.shape[1] + wk.shape[1] + wv.shape[1]
    flops = 2 * rows * (wq.shape[0] * cols + wo.shape[0] * wo.shape[1])
    kernel = functools.partial(block_kernel, parts=parts, seqs=seqs, seq_len=seq_len, chunk=512)
    vmem = pl.BlockSpec(memory_space=pltpu.VMEM)
    smem = pl.BlockSpec(memory_space=pltpu.SMEM)
    return pl.pallas_call(
        kernel,
        out_shape=[jax.ShapeDtypeStruct((rows, width), jnp.bfloat16)] * parts,
        in_specs=[smem, smem] + [vmem] * (parts + 7),
        out_specs=[vmem] * parts,
        scratch_shapes=[
            pltpu.VMEM((rows, cols), jnp.bfloat16),
            pltpu.VMEM((rows, wo.shape[0]), jnp.bfloat16),
        ],
        compiler_params=pltpu.CompilerParams(vmem_limit_bytes=GRANT),
        cost_estimate=pl.CostEstimate(flops=flops, transcendentals=0, bytes_accessed=rows * width * 8),
        name="block",
    )(place, lengths, *pieces, gain, *tables, *weights)


def merge_kernel(active_ref, own_ref, *refs):
    own = own_ref[...].astype(jnp.float32)
    total = refs[0][...].astype(jnp.float32)
    for ref in refs[1:-2]:
        total = total + ref[...].astype(jnp.float32)
    updated = (own + total).astype(jnp.bfloat16)
    refs[-2][...] = updated
    refs[-1][...] = jnp.where(active_ref[0] > 0, updated, own_ref[...])


def merge(active, own, terms):
    vmem = pl.BlockSpec(memory_space=pltpu.VMEM)
    return pl.pallas_call(
        merge_kernel,
        out_shape=[jax.ShapeDtypeStruct(own.shape, own.dtype)] * 2,
        in_specs=[pl.BlockSpec(memory_space=pltpu.SMEM)] + [vmem] * (1 + len(terms)),
        out_specs=[vmem] * 2,
        compiler_params=pltpu.CompilerParams(vmem_limit_bytes=GRANT // 2),
        name="merge",
    )(active, own, *terms)


def shards(
    support_tokens,
    support_lengths,
    support_labels,
    query_tokens,
    query_lengths,
    query_episodes,
    embedding,
    attn_gain,
    query_weight,
    key_weight,
    value_weight,
    out_weight,
    final_gain,
):
    both = ("dp", "pipe")
    group_count = lax.axis_size(both)
    replicas = lax.axis_size("dp")
    sections = lax.axis_size("pipe")
    parts = lax.axis_size("tensor")
    sup_dev, seq_len = support_tokens.shape
    qry_dev = query_tokens.shape[0]
    seq_count = sup_dev + qry_dev
    row_count = seq_count * seq_len
    table_rows, width = embedding.shape
    tensor_index = lax.axis_index("tensor")
    section_index = lax.axis_index("pipe")
    dp_index = lax.axis_index("dp")
    group_index = lax.axis_index(both)

    packed = jnp.concatenate(
        [
            support_tokens.reshape(-1),
            query_tokens.reshape(-1),
            support_lengths,
            query_lengths,
            support_labels.reshape(-1),
            query_episodes,
        ]
    )
    packed = jnp.pad(packed, (0, -packed.shape[0] % 128))
    everyone = lax.all_to_all(
        jnp.broadcast_to(packed[None, :], (group_count, packed.shape[0])), both, 0, 0, tiled=True
    )
    tokens = everyone[:, :row_count]
    lengths = everyone[:, row_count : row_count + seq_count]
    after = row_count + seq_count
    labels = everyone[:, after : after + sup_dev]
    episodes = everyone[:, after + sup_dev : after + sup_dev + qry_dev]

    positions = jnp.arange(seq_len)
    live = (positions[None, None, :] < lengths[:, :, None]).reshape(group_count, row_count)
    keys = jnp.where(live, tokens, -1)
    order = jnp.arange(row_count)
    earlier = order[None, :] < order[:, None]
    same = keys[:, :, None] == keys[:, None, :]
    first_at = jnp.min(jnp.where(same, order[None, None, :], row_count), axis=2)
    fresh = live & (first_at == order[None, :])
    owner = jnp.where(live, tokens // table_rows, -1)
    kin = (owner[:, :, None] == owner[:, None, :]) & fresh[:, None, :]
    rank = jnp.sum((kin & (order[None, None, :] < first_at[:, :, None])).astype(jnp.int32), axis=2)
    most = jnp.max(jnp.where(live, rank, -1)) + 1
    mine = fresh & (owner == group_index)
    local_rows = tokens - group_index * table_rows
    slots = jnp.arange(SLOTS)
    own_owner = lax.dynamic_slice_in_dim(owner, group_index, 1, 0)[0]
    own_rank = lax.dynamic_slice_in_dim(rank, group_index, 1, 0)[0]
    own_live = lax.dynamic_slice_in_dim(live, group_index, 1, 0)[0]

    def exchange(base):
        hit = mine[:, None, :] & (rank[:, None, :] == slots[None, :, None] + base)
        wanted = jnp.sum(jnp.where(hit, local_rows[:, None, :], 0), axis=2).reshape(-1)
        sent = jnp.take(embedding, wanted, axis=0, mode="clip")
        came = lax.all_to_all(sent, both, 0, 0, tiled=True)
        slot = own_rank - base
        good = own_live & (slot >= 0) & (slot < SLOTS)
        rows = jnp.take(came, jnp.where(good, own_owner * SLOTS + slot, 0), axis=0, mode="clip")
        return rows, good

    rows, good = exchange(0)
    hidden = jnp.where(good[:, None], rows, jnp.zeros_like(rows))

    def more(carry):
        return carry[0] < most

    def another(carry):
        base, held = carry
        rows, good = exchange(base)
        return base + SLOTS, jnp.where(good[:, None], rows, held)

    hidden = lax.cond(
        most > SLOTS,
        lambda held: lax.while_loop(more, another, (jnp.int32(SLOTS), held))[1],
        lambda held: held,
        hidden,
    )

    weights = (query_weight[0], key_weight[0], value_weight[0], out_weight[0])
    tables = rotary_tables(seq_len)
    place = tensor_index.astype(jnp.int32).reshape(1)
    dp_lengths = lax.dynamic_slice_in_dim(lengths, dp_index * sections, sections, 0)
    swaps = {
        k: [(i, (i + k) % parts) for i in range(parts)] for k in range(1, parts)
    }
    onward = [(i, (i + 1) % sections) for i in range(sections)]

    def spread(own):
        return [own] + [lax.ppermute(own, "tensor", swaps[k]) for k in range(1, parts)]

    streams = []
    for seqs in GROUPS:
        low, high = seqs[0] * seq_len, (seqs[-1] + 1) * seq_len
        streams.append(hidden[low:high])
    finished = [[None] * sections for _ in GROUPS]
    ticks = 2 * sections - 1
    tick_range = jnp.arange(ticks)
    active = ((section_index <= tick_range) & (tick_range < section_index + sections)).astype(jnp.int32)
    tick_lengths = jnp.take(dp_lengths, (section_index - tick_range) % sections, axis=0)
    actives = [active[t : t + 1] for t in range(ticks)]
    lengths_of = [[tick_lengths[t, g[0] : g[-1] + 1] for g in GROUPS] for t in range(ticks)]
    place, actives, lengths_of, streams, gain, tables = lax.optimization_barrier(
        (place, actives, lengths_of, streams, attn_gain, tables)
    )
    for tick in range(ticks):
        for j, seqs in enumerate(GROUPS):
            own = streams[j]
            pieces = spread(own)
            sums = block(place, lengths_of[tick][j], pieces, gain, tables, weights, seq_len)
            terms = [sums[0]] + [lax.ppermute(sums[k], "tensor", swaps[k]) for k in range(1, parts)]
            updated, going = merge(actives[tick], own, terms)
            if tick >= sections - 1:
                group = (sections - 1 - tick) % sections
                finished[j][group] = updated
            if tick < ticks - 1:
                streams[j] = lax.ppermute(going, "pipe", onward)

    done = jnp.concatenate(
        [finished[j][g].reshape(len(GROUPS[j]), seq_len, width) for g in range(sections) for j in range(len(GROUPS))],
        axis=0,
    ).astype(jnp.float32)
    square = jnp.sum(done * done, axis=2)
    full_square = square
    for k in range(1, parts):
        full_square = full_square + lax.ppermute(square, "tensor", swaps[k])
    done_lengths = dp_lengths.reshape(-1)
    done_live = (positions[None, :] < done_lengths[:, None]).astype(jnp.float32)
    factor = lax.rsqrt(full_square / (parts * width) + epsilon) * done_live
    gain_here = lax.dynamic_slice_in_dim(final_gain, tensor_index * width, width, 0)
    pooled = jnp.sum(done * factor[:, :, None], axis=1) * gain_here[None, :]
    pooled = (pooled / done_lengths[:, None].astype(jnp.float32)).astype(jnp.bfloat16)
    last = sections - 1
    shared = jnp.where(section_index == last, pooled, jnp.zeros_like(pooled))
    gathered = shared
    for z in range(last):
        gathered = gathered + lax.ppermute(shared, "pipe", [(last, z)])
    everything = lax.all_to_all(
        jnp.broadcast_to(gathered[None], (replicas,) + gathered.shape), "dp", 0, 0, tiled=True
    )
    everything = everything.reshape(group_count, seq_count, width).astype(jnp.float32)
    support_pooled = everything[:, :sup_dev].reshape(group_count * sup_dev, width)
    query_pooled = lax.dynamic_slice_in_dim(everything[:, sup_dev:], group_index, 1, 0)[0]
    own_episodes = lax.dynamic_slice_in_dim(episodes, group_index, 1, 0)[0]
    class_count_all = EPISODES * WAYS
    onehot = (labels.reshape(-1)[:, None] == jnp.arange(class_count_all)[None, :]).astype(jnp.float32)
    class_total = jnp.dot(onehot.T, support_pooled, precision=lax.Precision.HIGHEST)
    class_count = jnp.sum(onehot, axis=0)
    prototypes = class_total / class_count[:, None]
    by_episode = prototypes.reshape(EPISODES, WAYS, width)
    distances = []
    for e in range(EPISODES):
        distances.append(jnp.sum((query_pooled[:, None, :] - by_episode[e][None]) ** 2, axis=-1))
    distance = distances[0]
    for e in range(1, EPISODES):
        distance = jnp.where(own_episodes[:, None] == e, distances[e], distance)
    total = distance
    for k in range(1, parts):
        total = total + lax.ppermute(distance, "tensor", swaps[k])
    logits = -total / math.sqrt(D)
    return (prototypes, logits)


def solution(mesh):
    return jax.shard_map(
        shards,
        mesh=mesh,
        in_specs=(
            P(("dp", "pipe"), None),
            P(("dp", "pipe")),
            P(("dp", "pipe"), None),
            P(("dp", "pipe"), None),
            P(("dp", "pipe")),
            P(("dp", "pipe")),
            P(("dp", "pipe"), "tensor"),
            P("pipe", None),
            P("pipe", None, "tensor"),
            P("pipe", None, "tensor"),
            P("pipe", None, "tensor"),
            P("pipe", "tensor", None),
            P(),
        ),
        out_specs=(P(None, "tensor"), P(("dp", "pipe"), None)),
        check_vma=False,
    )
```

```python
import functools
import math

import jax
import jax.numpy as jnp
from jax import lax
from jax.experimental import pallas as pl
from jax.experimental.pallas import tpu as pltpu
from jax.sharding import PartitionSpec as P

D = 4096
HEAD_DIM = 128
WAYS = 16
EPISODES = 2
GRANT = 6 * 1024 * 1024
SLOTS = 16
PIECES = 3

epsilon = 1e-05
rotary_base = 500000.0


def rotary_tables(seq_len):
    half_dim = HEAD_DIM // 2
    freqs = jnp.exp(
        -math.log(rotary_base) * jnp.arange(half_dim, dtype=jnp.float32) * (2.0 / HEAD_DIM)
    )
    angles = jnp.arange(seq_len, dtype=jnp.float32)[:, None] * freqs[None, :]
    cosine, sine = jnp.cos(angles), jnp.sin(angles)
    return (
        jnp.concatenate([cosine, cosine], axis=1),
        jnp.concatenate([-sine, sine], axis=1),
    )


def block_kernel(
    place_ref,
    lengths_ref,
    *refs,
    parts,
    pieces,
    seqs,
    seq_len,
    chunk,
):
    rows_refs = [refs[k * pieces : (k + 1) * pieces] for k in range(parts)]
    refs = refs[parts * pieces :]
    gain_ref, cos_ref, sin_ref, wq_ref, wk_ref, wv_ref, wo_ref = refs[:7]
    mixed_ref = refs[7]
    out_refs = [refs[8 + k * pieces : 8 + (k + 1) * pieces] for k in range(parts - 1)]
    qkv_ref = refs[8 + (parts - 1) * pieces]
    width = rows_refs[0][0].shape[1]
    here = place_ref[0]
    starts = [pl.multiple_of(lax.rem(here + parts - k, parts) * width, width) for k in range(parts)]
    values = [
        jnp.concatenate([ref[...] for ref in part], axis=0).astype(jnp.float32) for part in rows_refs
    ]
    total = jnp.sum(values[0] * values[0], axis=1, keepdims=True)
    for part in values[1:]:
        total = total + jnp.sum(part * part, axis=1, keepdims=True)
    scale = lax.rsqrt(total / (parts * width) + epsilon)
    normed = []
    for part, start in zip(values, starts):
        gain = gain_ref[:, pl.ds(start, width)]
        normed.append((part * scale * gain).astype(jnp.bfloat16))
    query_cols = wq_ref.shape[1]
    key_cols = wk_ref.shape[1]
    cosine = jnp.concatenate([cos_ref[...]] * seqs, axis=0)
    sine = jnp.concatenate([sin_ref[...]] * seqs, axis=0)

    def project(weight_ref, base, turned):
        cols = weight_ref.shape[1]
        step = min(chunk, cols)
        for at in range(0, cols, step):
            acc = None
            for part, start in zip(normed, starts):
                term = jnp.dot(
                    part,
                    weight_ref[pl.ds(start, width), at : at + step],
                    preferred_element_type=jnp.float32,
                )
                acc = term if acc is None else acc + term
            for low in range(0, step, HEAD_DIM):
                head = acc[:, low : low + HEAD_DIM]
                if turned:
                    head = head * cosine + pltpu.roll(head, HEAD_DIM // 2, 1) * sine
                qkv_ref[:, base + at + low : base + at + low + HEAD_DIM] = head.astype(jnp.bfloat16)

    project(wk_ref, query_cols, True)
    project(wv_ref, query_cols + key_cols, False)
    project(wq_ref, 0, True)
    heads = query_cols // HEAD_DIM
    groups = key_cols // HEAD_DIM
    each = heads // groups
    spot = lax.broadcasted_iota(jnp.int32, (each * seq_len, seq_len), 0) % seq_len
    seen = lax.broadcasted_iota(jnp.int32, (each * seq_len, seq_len), 1)
    for s in range(seqs):
        at = slice(s * seq_len, (s + 1) * seq_len)
        visible = (seen <= spot) & (seen < lengths_ref[s])
        for g in range(groups):
            query = jnp.concatenate(
                [
                    qkv_ref[at, (g * each + i) * HEAD_DIM : (g * each + i + 1) * HEAD_DIM]
                    for i in range(each)
                ],
                axis=0,
            )
            key = qkv_ref[at, query_cols + g * HEAD_DIM : query_cols + (g + 1) * HEAD_DIM]
            base = query_cols + key_cols
            value = qkv_ref[at, base + g * HEAD_DIM : base + (g + 1) * HEAD_DIM]
            scores = lax.dot_general(
                query, key, (((1,), (1,)), ((), ())), preferred_element_type=jnp.float32
            ) * (1.0 / math.sqrt(HEAD_DIM))
            scores = jnp.where(visible, scores, -1e30)
            top = jnp.max(scores, axis=1, keepdims=True)
            powers = jnp.exp(scores - top)
            weights = (powers / jnp.sum(powers, axis=1, keepdims=True)).astype(jnp.bfloat16)
            mixed = jnp.dot(weights, value, preferred_element_type=jnp.float32).astype(jnp.bfloat16)
            for i in range(each):
                low = (g * each + i) * HEAD_DIM
                mixed_ref[at, low : low + HEAD_DIM] = mixed[i * seq_len : (i + 1) * seq_len]
    mixed = mixed_ref[...]
    for k in range(1, parts):
        to = pl.multiple_of(lax.rem(here + k, parts) * width, width)
        for low in range(0, width, chunk):
            part = jnp.dot(
                mixed, wo_ref[:, pl.ds(to + low, chunk)], preferred_element_type=jnp.float32
            ).astype(jnp.bfloat16)
            at = 0
            for ref in out_refs[k - 1]:
                ref[:, low : low + chunk] = part[at : at + ref.shape[0]]
                at += ref.shape[0]


def keep_kernel(place_ref, mixed_ref, wo_ref, out_ref, *, chunk):
    width = out_ref.shape[1]
    to = pl.multiple_of(place_ref[0] * width, width)
    mixed = mixed_ref[...]
    for low in range(0, width, chunk):
        out_ref[:, low : low + chunk] = jnp.dot(
            mixed, wo_ref[:, pl.ds(to + low, chunk)], preferred_element_type=jnp.float32
        ).astype(jnp.bfloat16)


def block(place, lengths, features, gain, tables, weights, seq_len):
    parts = len(features)
    pieces = len(features[0])
    heights = [piece.shape[0] for piece in features[0]]
    rows, width = sum(heights), features[0][0].shape[1]
    wq, wk, wv, wo = weights
    cols = wq.shape[1] + wk.shape[1] + wv.shape[1]
    kernel = functools.partial(
        block_kernel, parts=parts, pieces=pieces, seqs=rows // seq_len, seq_len=seq_len, chunk=512
    )
    vmem = pl.BlockSpec(memory_space=pltpu.VMEM)
    smem = pl.BlockSpec(memory_space=pltpu.SMEM)
    shape = functools.partial(jax.ShapeDtypeStruct, dtype=jnp.bfloat16)
    outs = pl.pallas_call(
        kernel,
        out_shape=[shape((rows, wo.shape[0]))] + [shape((h, width)) for h in heights] * (parts - 1),
        in_specs=[smem, smem] + [vmem] * (parts * pieces + 7),
        out_specs=[vmem] * (1 + pieces * (parts - 1)),
        scratch_shapes=[pltpu.VMEM((rows, cols), jnp.bfloat16)],
        compiler_params=pltpu.CompilerParams(vmem_limit_bytes=GRANT),
        cost_estimate=pl.CostEstimate(
            flops=2 * rows * wq.shape[0] * cols, transcendentals=0, bytes_accessed=rows * width * 8
        ),
        name="block",
    )(place, lengths, *[piece for part in features for piece in part], gain, *tables, *weights)
    mixed, sent = outs[0], outs[1:]
    kept = pl.pallas_call(
        functools.partial(keep_kernel, chunk=512),
        out_shape=shape((rows, width)),
        in_specs=[smem, vmem, vmem],
        out_specs=vmem,
        compiler_params=pltpu.CompilerParams(vmem_limit_bytes=GRANT),
        cost_estimate=pl.CostEstimate(
            flops=2 * rows * wo.shape[0] * width, transcendentals=0, bytes_accessed=rows * width * 8
        ),
        name="keep",
    )(place, mixed, wo)
    return kept, [sent[k * pieces : (k + 1) * pieces] for k in range(parts - 1)]


def merge_kernel(active_ref, own_ref, kept_ref, *refs, low):
    rows = own_ref.shape[0]
    own = own_ref[...]
    total = kept_ref[low : low + rows, :].astype(jnp.float32)
    for ref in refs[:-1]:
        total = total + ref[...].astype(jnp.float32)
    updated = (own.astype(jnp.float32) + total).astype(jnp.bfloat16)
    refs[-1][...] = jnp.where(active_ref[0] > 0, updated, own)


def merge(active, own, kept, terms, low):
    vmem = pl.BlockSpec(memory_space=pltpu.VMEM)
    return pl.pallas_call(
        functools.partial(merge_kernel, low=low),
        out_shape=jax.ShapeDtypeStruct(own.shape, own.dtype),
        in_specs=[pl.BlockSpec(memory_space=pltpu.SMEM)] + [vmem] * (2 + len(terms)),
        out_specs=vmem,
        compiler_params=pltpu.CompilerParams(vmem_limit_bytes=GRANT // 2),
        name="merge",
    )(active, own, kept, *terms)


def shards(
    support_tokens,
    support_lengths,
    support_labels,
    query_tokens,
    query_lengths,
    query_episodes,
    embedding,
    attn_gain,
    query_weight,
    key_weight,
    value_weight,
    out_weight,
    final_gain,
):
    both = ("dp", "pipe")
    group_count = lax.axis_size(both)
    replicas = lax.axis_size("dp")
    sections = lax.axis_size("pipe")
    parts = lax.axis_size("tensor")
    sup_dev, seq_len = support_tokens.shape
    qry_dev = query_tokens.shape[0]
    seq_count = sup_dev + qry_dev
    row_count = seq_count * seq_len
    table_rows, width = embedding.shape
    tensor_index = lax.axis_index("tensor")
    section_index = lax.axis_index("pipe")
    dp_index = lax.axis_index("dp")
    group_index = lax.axis_index(both)

    packed = jnp.concatenate(
        [
            support_tokens.reshape(-1),
            query_tokens.reshape(-1),
            support_lengths,
            query_lengths,
            support_labels.reshape(-1),
            query_episodes,
        ]
    )
    packed = jnp.pad(packed, (0, -packed.shape[0] % 128))
    everyone = lax.all_to_all(
        jnp.broadcast_to(packed[None, :], (group_count, packed.shape[0])), both, 0, 0, tiled=True
    )
    tokens = everyone[:, :row_count]
    lengths = everyone[:, row_count : row_count + seq_count]
    after = row_count + seq_count
    labels = everyone[:, after : after + sup_dev]
    episodes = everyone[:, after + sup_dev : after + sup_dev + qry_dev]

    positions = jnp.arange(seq_len)
    live = (positions[None, None, :] < lengths[:, :, None]).reshape(group_count, row_count)
    keys = jnp.where(live, tokens, -1)
    order = jnp.arange(row_count)
    earlier = order[None, :] < order[:, None]
    same = keys[:, :, None] == keys[:, None, :]
    first_at = jnp.min(jnp.where(same, order[None, None, :], row_count), axis=2)
    fresh = live & (first_at == order[None, :])
    owner = jnp.where(live, tokens // table_rows, -1)
    kin = (owner[:, :, None] == owner[:, None, :]) & fresh[:, None, :]
    rank = jnp.sum((kin & (order[None, None, :] < first_at[:, :, None])).astype(jnp.int32), axis=2)
    most = jnp.max(jnp.where(live, rank, -1)) + 1
    mine = fresh & (owner == group_index)
    local_rows = tokens - group_index * table_rows
    slots = jnp.arange(SLOTS)
    own_owner = lax.dynamic_slice_in_dim(owner, group_index, 1, 0)[0]
    own_rank = lax.dynamic_slice_in_dim(rank, group_index, 1, 0)[0]
    own_live = lax.dynamic_slice_in_dim(live, group_index, 1, 0)[0]

    def exchange(base):
        hit = mine[:, None, :] & (rank[:, None, :] == slots[None, :, None] + base)
        wanted = jnp.sum(jnp.where(hit, local_rows[:, None, :], 0), axis=2).reshape(-1)
        sent = jnp.take(embedding, wanted, axis=0, mode="clip")
        came = lax.all_to_all(sent, both, 0, 0, tiled=True)
        slot = own_rank - base
        good = own_live & (slot >= 0) & (slot < SLOTS)
        rows = jnp.take(came, jnp.where(good, own_owner * SLOTS + slot, 0), axis=0, mode="clip")
        return rows, good

    rows, good = exchange(0)
    hidden = jnp.where(good[:, None], rows, jnp.zeros_like(rows))

    def more(carry):
        return carry[0] < most

    def another(carry):
        base, held = carry
        rows, good = exchange(base)
        return base + SLOTS, jnp.where(good[:, None], rows, held)

    hidden = lax.cond(
        most > SLOTS,
        lambda held: lax.while_loop(more, another, (jnp.int32(SLOTS), held))[1],
        lambda held: held,
        hidden,
    )

    weights = (query_weight[0], key_weight[0], value_weight[0], out_weight[0])
    tables = rotary_tables(seq_len)
    place = tensor_index.astype(jnp.int32).reshape(1)
    dp_lengths = lax.dynamic_slice_in_dim(lengths, dp_index * sections, sections, 0)
    swaps = {
        k: [(i, (i + k) % parts) for i in range(parts)] for k in range(1, parts)
    }
    onward = [(i, (i + 1) % sections) for i in range(sections)]

    cuts = [row_count * i // PIECES // 16 * 16 for i in range(PIECES)] + [row_count]
    stream = [hidden[cuts[i] : cuts[i + 1]] for i in range(PIECES)]
    finished = [None] * sections
    ticks = 2 * sections - 1
    tick_range = jnp.arange(ticks)
    active = (section_index <= tick_range).astype(jnp.int32)
    tick_lengths = jnp.take(dp_lengths, (section_index - tick_range) % sections, axis=0)
    actives = [active[t : t + 1] for t in range(ticks)]
    lengths_of = [tick_lengths[t] for t in range(ticks)]
    place, actives, lengths_of, stream, gain, tables = lax.optimization_barrier(
        (place, actives, lengths_of, stream, attn_gain, tables)
    )
    for tick in range(ticks):
        features = [stream] + [
            [lax.ppermute(piece, "tensor", swaps[k]) for piece in stream] for k in range(1, parts)
        ]
        kept, sent = block(place, lengths_of[tick], features, gain, tables, weights, seq_len)
        moved = []
        for i in range(PIECES):
            terms = [lax.ppermute(sent[k - 1][i], "tensor", swaps[k]) for k in range(1, parts)]
            moved.append(merge(actives[tick], stream[i], kept, terms, cuts[i]))
        if tick >= sections - 1:
            finished[(sections - 1 - tick) % sections] = moved
        if tick < ticks - 1:
            stream = [lax.ppermute(piece, "pipe", onward) for piece in moved]

    done = jnp.concatenate([piece for ended in finished for piece in ended], axis=0)
    done = done.reshape(sections * seq_count, seq_len, width).astype(jnp.float32)
    square = jnp.sum(done * done, axis=2)
    full_square = square
    for k in range(1, parts):
        full_square = full_square + lax.ppermute(square, "tensor", swaps[k])
    done_lengths = dp_lengths.reshape(-1)
    done_live = (positions[None, :] < done_lengths[:, None]).astype(jnp.float32)
    factor = lax.rsqrt(full_square / (parts * width) + epsilon) * done_live
    gain_here = lax.dynamic_slice_in_dim(final_gain, tensor_index * width, width, 0)
    pooled = jnp.sum(done * factor[:, :, None], axis=1) * gain_here[None, :]
    pooled = (pooled / done_lengths[:, None].astype(jnp.float32)).astype(jnp.bfloat16)
    last = sections - 1
    shared = jnp.where(section_index == last, pooled, jnp.zeros_like(pooled))
    gathered = shared
    for z in range(last):
        gathered = gathered + lax.ppermute(shared, "pipe", [(last, z)])
    everything = lax.all_to_all(
        jnp.broadcast_to(gathered[None], (replicas,) + gathered.shape), "dp", 0, 0, tiled=True
    )
    everything = everything.reshape(group_count, seq_count, width).astype(jnp.float32)
    support_pooled = everything[:, :sup_dev].reshape(group_count * sup_dev, width)
    query_pooled = lax.dynamic_slice_in_dim(everything[:, sup_dev:], group_index, 1, 0)[0]
    own_episodes = lax.dynamic_slice_in_dim(episodes, group_index, 1, 0)[0]
    class_count_all = EPISODES * WAYS
    onehot = (labels.reshape(-1)[:, None] == jnp.arange(class_count_all)[None, :]).astype(jnp.float32)
    class_total = jnp.dot(onehot.T, support_pooled, precision=lax.Precision.HIGHEST)
    class_count = jnp.sum(onehot, axis=0)
    prototypes = class_total / class_count[:, None]
    by_episode = prototypes.reshape(EPISODES, WAYS, width)
    distances = []
    for e in range(EPISODES):
        distances.append(jnp.sum((query_pooled[:, None, :] - by_episode[e][None]) ** 2, axis=-1))
    distance = distances[0]
    for e in range(1, EPISODES):
        distance = jnp.where(own_episodes[:, None] == e, distances[e], distance)
    total = distance
    for k in range(1, parts):
        total = total + lax.ppermute(distance, "tensor", swaps[k])
    logits = -total / math.sqrt(D)
    return (prototypes, logits)


def solution(mesh):
    return jax.shard_map(
        shards,
        mesh=mesh,
        in_specs=(
            P(("dp", "pipe"), None),
            P(("dp", "pipe")),
            P(("dp", "pipe"), None),
            P(("dp", "pipe"), None),
            P(("dp", "pipe")),
            P(("dp", "pipe")),
            P(("dp", "pipe"), "tensor"),
            P("pipe", None),
            P("pipe", None, "tensor"),
            P("pipe", None, "tensor"),
            P("pipe", None, "tensor"),
            P("pipe", "tensor", None),
            P(),
        ),
        out_specs=(P(None, "tensor"), P(("dp", "pipe"), None)),
        check_vma=False,
    )
```
